32 devices in a mesh: row: 4 (over z), col: 8 (over y, x, core).
Axes of the slice: x: 2, y: 2, z: 4, core: 2. Of those that a mesh axis runs over, the one named last changes fastest.
Arguments:
- diag_blocks: float32 [8, 16, 512, 512], P('row', 'col'), may hold values from -4 to 16, as said below
- horizontal: bfloat16 [8, 16, 512, 512], P('row', 'col'), may hold values from -0.125 to 0.125
- vertical: bfloat16 [8, 16, 512, 512], P('row', 'col'), may hold values from -0.125 to 0.125
Outputs:
- red_factor: float32 [8, 8, 512, 512], P('row', 'col')
- black_schur: float32 [8, 8, 512, 512], P('row', 'col')
- black_links: bfloat16 [8, 8, 4, 512, 512], P('row', 'col')
The draws below stay inside these ranges and needn't reach their ends.
Inputs may be any that keep to these rules, and one draw needn't show every extreme that they name: `diag_blocks`: every block is symmetric and its eigenvalues are at least 1.
All inputs are finite; a program needn't handle non-finite values.
Results may differ from the reference program's by a relative error of at most 0.0054.
Values may be sent and summed in bfloat16 or wider, within the bound.
A program may use at most 128 MiB of HBM per device.

```python
import math
import jax
import jax.numpy as jnp
from jax import lax

BLOCK = 512
GRID_ROWS = 8
GRID_COLS = 16


def draw_diag_blocks(key, part):
    first_key = jax.random.fold_in(key, 11)
    second_key = jax.random.fold_in(key, 12)
    factor = jax.random.normal(first_key, (GRID_ROWS, GRID_COLS, BLOCK, BLOCK), jnp.float32)
    levels = jnp.exp(jax.random.uniform(second_key, (GRID_ROWS, GRID_COLS, BLOCK), jnp.float32, 0.0, math.log(4.0)))
    strength = 2.0
    gram = jnp.einsum('rcik,rcjk->rcij', factor, factor, precision=lax.Precision.HIGHEST) * (strength / BLOCK)
    return gram + levels[..., None] * jnp.eye(BLOCK, dtype=jnp.float32)


def block_levels(rng, dims, split, smallest, top_value):
    def one(position, parts):
        heights = jax.random.uniform(jax.random.fold_in(jax.random.fold_in(rng, 6), position), (parts,), jnp.float32, smallest / len(split), top_value / len(split))
        return jnp.repeat(jnp.exp(heights), dims[position] // parts).reshape((-1,) + (1,) * (len(dims) - position - 1))

    level = one(*split[0])
    for cut in split[1:]:
        level = level * one(*cut)
    return level


def gaussian(rng, shape, width, most, pieces=(), kind=jnp.bfloat16):
    factor_of = block_levels(rng, shape, pieces, -0.22, 0.18) if pieces else 1.0
    drawn = jax.random.normal(rng, shape, jnp.float32) * width * factor_of
    return jnp.minimum(jnp.maximum(drawn, -most), most).astype(kind)


def setup_inputs(seed: int = 0) -> dict:
    keys = jax.random.split(jax.random.key(seed), 4)
    diag_blocks = draw_diag_blocks(jax.random.fold_in(keys[3], 71), 0)
    horizontal = gaussian(keys[1], (GRID_ROWS, GRID_COLS, BLOCK, BLOCK), (4 * BLOCK) ** -0.5, 0.125, ((0, 4), (1, 8)))
    vertical = gaussian(keys[2], (GRID_ROWS, GRID_COLS, BLOCK, BLOCK), (4 * BLOCK) ** -0.5, 0.125, ((0, 4), (1, 8)))
    return dict(diag_blocks=diag_blocks, horizontal=horizontal, vertical=vertical)


def select_colour(blocks, parity):
    grid_rows = blocks.shape[0]
    grid_columns = blocks.shape[1]
    trailing = blocks.shape[2:]
    paired = blocks.reshape((grid_rows // 2, 2, grid_columns // 2, 2) + trailing)
    joined = jnp.stack([paired[:, 0, :, parity], paired[:, 1, :, 1 - parity]], 1)
    return joined.reshape((grid_rows, grid_columns // 2) + trailing)

def combine_rows(even_rows, odd_rows):
    joined = jnp.stack([even_rows, odd_rows], 1)
    return joined.reshape((2 * even_rows.shape[0],) + even_rows.shape[1:])

def transposed(blocks):
    return jnp.swapaxes(blocks, -1, -2)

def gram_term(former, latter):
    return jnp.einsum('mka,mkb->mab', former.astype(jnp.float32), latter.astype(jnp.float32), precision=lax.Precision.HIGHEST)

def solve_red(packed):
    factor = jnp.linalg.cholesky(packed[0])
    results = [jax.scipy.linalg.solve_triangular(factor, coupling, lower=True) for coupling in packed[1:]]
    return (factor, jnp.stack(results, 1).astype(jnp.bfloat16))

def black_row(packed):
    diag_black, above, below, left_red, right_red = packed
    update = gram_term(above[:, 3], above[:, 3]) + gram_term(below[:, 1], below[:, 1])
    update = update + gram_term(left_red[:, 2], left_red[:, 2]) + gram_term(right_red[:, 0], right_red[:, 0])
    schur_part = diag_black - update
    east_link = -gram_term(right_red[:, 0], right_red[:, 2])
    south_link = -gram_term(below[:, 1], below[:, 3])
    southeast = -(gram_term(right_red[:, 0], right_red[:, 3]) + gram_term(below[:, 1], below[:, 2]))
    southwest = -(gram_term(left_red[:, 2], left_red[:, 3]) + gram_term(below[:, 1], below[:, 0]))
    links = jnp.stack([east_link, south_link, southeast, southwest], 1).astype(jnp.bfloat16)
    return (schur_part, links)

def reference(diag_blocks, horizontal, vertical):
    left_links = jnp.roll(horizontal, 1, axis=1)
    upper_links = jnp.roll(vertical, 1, axis=0)
    couplings = (transposed(select_colour(left_links, 0)).astype(jnp.float32), transposed(select_colour(upper_links, 0)).astype(jnp.float32), select_colour(horizontal, 0).astype(jnp.float32), select_colour(vertical, 0).astype(jnp.float32))
    red_factor, solved = lax.map(solve_red, (select_colour(diag_blocks, 0),) + couplings)
    above = jnp.roll(solved, 1, axis=0)
    below = jnp.roll(solved, -1, axis=0)
    previous = jnp.roll(solved, 1, axis=1)
    following = jnp.roll(solved, -1, axis=1)
    left_red = combine_rows(solved[0::2], previous[1::2])
    right_red = combine_rows(following[0::2], solved[1::2])
    black_schur, black_links = lax.map(black_row, (select_colour(diag_blocks, 1), above, below, left_red, right_red))
    return (red_factor, black_schur, black_links)
```

```python
import functools

import jax
import jax.numpy as jnp
from jax import lax
from jax.experimental import pallas as pl
from jax.experimental.pallas import tpu as pltpu
from jax.sharding import PartitionSpec as P

PANEL = 128
STRIP = 8
VMEM = pl.BlockSpec(memory_space=pltpu.VMEM)


def split(value):
    high = value.astype(jnp.bfloat16)
    low = (value - high.astype(jnp.float32)).astype(jnp.bfloat16)
    return high, low


def product(left, right):
    dot = functools.partial(jnp.dot, preferred_element_type=jnp.float32)
    (lh, ll), (rh, rl) = left, right
    return dot(lh, rh) + (dot(lh, rl) + dot(ll, rh))


def factor_diagonal(work, count):
    lane = lax.broadcasted_iota(jnp.int32, (STRIP, PANEL), 1)
    sub = lax.broadcasted_iota(jnp.int32, (STRIP, PANEL), 0)
    sub_wide = lax.broadcasted_iota(jnp.int32, (STRIP, 2 * PANEL), 0)

    def strip(b, carry):
        start = pl.multiple_of(b * STRIP, STRIP)
        rows = [work[m, pl.ds(start, STRIP), :] for m in range(count)]
        columns = [
            [
                jnp.take_along_axis(rows[m][:, :PANEL], jnp.full_like(lane, start + c), axis=1)
                for c in range(STRIP)
            ]
            for m in range(count)
        ]
        for j in range(STRIP):
            for m in range(count):
                column = columns[m][j]
                pivot = jnp.broadcast_to(column[j : j + 1], column.shape)
                root = lax.rsqrt(pivot)
                square = root * root
                below = jnp.where(sub > j, column, 0.0)
                for c in range(j + 1, STRIP):
                    across = jnp.broadcast_to(columns[m][c][j : j + 1], column.shape)
                    columns[m][c] = columns[m][c] - (below * across) * square
                row = jnp.broadcast_to(rows[m][j : j + 1], rows[m].shape)
                wide_below = jnp.concatenate([below * square] * 2, 1)
                wide_root = jnp.concatenate([root] * 2, 1)
                rows[m] = jnp.where(sub_wide == j, row * wide_root, rows[m] - wide_below * row)
        for m in range(count):
            work[m, pl.ds(start, STRIP), :] = rows[m]
            high = rows[m].astype(jnp.bfloat16).astype(jnp.float32)
            low = rows[m] - high
            after = lane >= start + STRIP
            left_high = jnp.where(after, high[:, :PANEL], 0.0)
            left_low = jnp.where(after, low[:, :PANEL], 0.0)
            left = jnp.concatenate([left_high, left_high, left_low, left_low], 0)
            right = jnp.concatenate([high, low, high, low], 0)
            work[m] = work[m] - lax.dot_general(
                left.T.astype(jnp.bfloat16),
                right.astype(jnp.bfloat16),
                (((1,), (0,)), ((), ())),
                preferred_element_type=jnp.float32,
            )
        return carry

    lax.fori_loop(0, PANEL // STRIP, strip, 0)


def factor_kernel(diag, factor, inverse, blocks, work):
    count, order = diag.shape[0], diag.shape[1]
    row = lax.broadcasted_iota(jnp.int32, (PANEL, PANEL), 0)
    col = lax.broadcasted_iota(jnp.int32, (PANEL, PANEL), 1)
    eye = jnp.where(row == col, 1.0, 0.0).astype(jnp.float32)
    blocks[...] = diag[...]
    inverse[...] = jnp.zeros_like(inverse)
    factor[...] = jnp.zeros_like(factor)
    for start in range(0, order, PANEL):
        stop = start + PANEL
        here = slice(start, stop)
        for m in range(count):
            work[m, :, :PANEL] = blocks[m, here, here]
            work[m, :, PANEL:] = eye
        factor_diagonal(work, count)
        for m in range(count):
            upper = jnp.where(col >= row, work[m, :, :PANEL], 0.0)
            factor[m, here, here] = upper.T
            small = jnp.where(col <= row, work[m, :, PANEL:], 0.0)
            small_parts = split(small)
            if start:
                inverse[m, here, :start] = product(small_parts, split(inverse[m, here, :start]))
            inverse[m, here, here] = small
            if stop < order:
                across = product(small_parts, split(blocks[m, here, stop:]))
                down = across.T
                factor[m, stop:, here] = down
                down_parts = split(down)
                blocks[m, stop:, stop:] -= product(down_parts, split(across))
                inverse[m, stop:, :stop] -= product(down_parts, split(inverse[m, here, :stop]))


def factored(diag):
    shape = jax.ShapeDtypeStruct(diag.shape, jnp.float32)
    return pl.pallas_call(
        factor_kernel,
        out_shape=(shape, shape),
        in_specs=[VMEM],
        out_specs=(VMEM, VMEM),
        scratch_shapes=[
            pltpu.VMEM(diag.shape, jnp.float32),
            pltpu.VMEM((diag.shape[0], PANEL, 2 * PANEL), jnp.float32),
        ],
        compiler_params=pltpu.CompilerParams(vmem_limit_bytes=40 * 2**20),
        cost_estimate=pl.CostEstimate(
            flops=20_000_000_000, bytes_accessed=3 * diag.size * 4, transcendentals=0
        ),
    )(diag)


def passed_along(value, axis, by):
    size = lax.axis_size(axis)
    return lax.ppermute(value, axis, [(i, (i + by) % size) for i in range(size)])


def select_colour(blocks, parity):
    grid_rows = blocks.shape[0]
    grid_columns = blocks.shape[1]
    trailing = blocks.shape[2:]
    paired = blocks.reshape((grid_rows // 2, 2, grid_columns // 2, 2) + trailing)
    joined = jnp.stack([paired[:, 0, :, parity], paired[:, 1, :, 1 - parity]], 1)
    return joined.reshape((grid_rows, grid_columns // 2) + trailing)


def combine_rows(even_rows, odd_rows):
    joined = jnp.stack([even_rows, odd_rows], 1)
    return joined.reshape((2 * even_rows.shape[0],) + even_rows.shape[1:])


def transposed(blocks):
    return jnp.swapaxes(blocks, -1, -2)


def gram_term(former, latter):
    return jnp.einsum("rmka,rmkb->rmab", former, latter, preferred_element_type=jnp.float32)


def solve(inverse, coupling, axes):
    high, low = split(inverse)
    dot = functools.partial(jnp.einsum, axes, preferred_element_type=jnp.float32)
    return dot(high, coupling) + dot(low, coupling)


def on_device(diag_blocks, horizontal, vertical):
    rows, half = diag_blocks.shape[0], diag_blocks.shape[1] // 2
    block = diag_blocks.shape[2:]
    edge_column = passed_along(horizontal[:, -1:], "col", 1)
    left_links = jnp.concatenate([edge_column, horizontal[:, :-1]], 1)
    edge_row = passed_along(vertical[-1:], "row", 1)
    upper_links = jnp.concatenate([edge_row, vertical[:-1]], 0)
    red_factor, inverse = factored(select_colour(diag_blocks, 0).reshape((-1,) + block))
    inverse = inverse.reshape((rows, half) + block)
    solved = jnp.stack(
        [
            solve(inverse, select_colour(left_links, 0), "rmab,rmcb->rmac"),
            solve(inverse, select_colour(upper_links, 0), "rmab,rmcb->rmac"),
            solve(inverse, select_colour(horizontal, 0), "rmab,rmbc->rmac"),
            solve(inverse, select_colour(vertical, 0), "rmab,rmbc->rmac"),
        ],
        2,
    ).astype(jnp.bfloat16)
    red_factor = red_factor.reshape((rows, half) + block)
    got_above = passed_along(solved[-1:, :, 3], "row", 1)
    above_down = jnp.concatenate([got_above, solved[:-1, :, 3]], 0)
    got_below = passed_along(solved[:1], "row", -1)
    below_all = jnp.concatenate([solved[1:], got_below], 0)
    got_left = passed_along(solved[1::2, -1:, 2:4], "col", 1)
    left_pair = combine_rows(
        solved[0::2, :, 2:4], jnp.concatenate([got_left, solved[1::2, :-1, 2:4]], 1)
    )
    right_first, right_rest = passed_along((solved[0::2, :1, 0], solved[0::2, :1, 2:4]), "col", -1)
    right_left = combine_rows(
        jnp.concatenate([solved[0::2, 1:, 0], right_first], 1), solved[1::2, :, 0]
    )
    right_pair = combine_rows(
        jnp.concatenate([solved[0::2, 1:, 2:4], right_rest], 1), solved[1::2, :, 2:4]
    )
    below_up = below_all[:, :, 1]
    update = gram_term(above_down, above_down) + gram_term(below_up, below_up)
    update = (
        update
        + gram_term(left_pair[:, :, 0], left_pair[:, :, 0])
        + gram_term(right_left, right_left)
    )
    black_schur = select_colour(diag_blocks, 1) - update
    east_link = -gram_term(right_left, right_pair[:, :, 0])
    south_link = -gram_term(below_up, below_all[:, :, 3])
    southeast = -(
        gram_term(right_left, right_pair[:, :, 1]) + gram_term(below_up, below_all[:, :, 2])
    )
    southwest = -(
        gram_term(left_pair[:, :, 0], left_pair[:, :, 1]) + gram_term(below_up, below_all[:, :, 0])
    )
    black_links = jnp.stack([east_link, south_link, southeast, southwest], 2).astype(jnp.bfloat16)
    return (red_factor, black_schur, black_links)


def solution(mesh):
    in_specs = (
        P("row", "col", None, None),
        P("row", "col", None, None),
        P("row", "col", None, None),
    )
    out_specs = (
        P("row", "col", None, None),
        P("row", "col", None, None),
        P("row", "col", None, None, None),
    )
    return jax.shard_map(
        on_device, mesh=mesh, in_specs=in_specs, out_specs=out_specs, check_vma=False
    )
```

```python
import functools

import jax
import jax.numpy as jnp
from jax import lax
from jax.experimental import pallas as pl
from jax.experimental.pallas import tpu as pltpu
from jax.sharding import PartitionSpec as P

PANEL = 128
STRIP = 8
VMEM = pl.BlockSpec(memory_space=pltpu.VMEM)


def split(value):
    high = value.astype(jnp.bfloat16)
    low = (value - high.astype(jnp.float32)).astype(jnp.bfloat16)
    return high, low


def product(left, right):
    dot = functools.partial(jnp.dot, preferred_element_type=jnp.float32)
    (lh, ll), (rh, rl) = left, right
    return dot(lh, rh) + (dot(lh, rl) + dot(ll, rh))


def factor_diagonal(work, count):
    lane = lax.broadcasted_iota(jnp.int32, (STRIP, PANEL), 1)
    sub = lax.broadcasted_iota(jnp.int32, (STRIP, PANEL), 0)
    sub_wide = lax.broadcasted_iota(jnp.int32, (STRIP, 2 * PANEL), 0)

    def strip(b, carry):
        start = pl.multiple_of(b * STRIP, STRIP)
        rows = [work[m, pl.ds(start, STRIP), :] for m in range(count)]
        columns = [
            [
                jnp.take_along_axis(rows[m][:, :PANEL], jnp.full_like(lane, start + c), axis=1)
                for c in range(STRIP)
            ]
            for m in range(count)
        ]
        for j in range(STRIP):
            for m in range(count):
                column = columns[m][j]
                pivot = jnp.broadcast_to(column[j : j + 1], column.shape)
                root = lax.rsqrt(pivot)
                square = root * root
                below = jnp.where(sub > j, column, 0.0)
                for c in range(j + 1, STRIP):
                    across = jnp.broadcast_to(columns[m][c][j : j + 1], column.shape)
                    columns[m][c] = columns[m][c] - (below * across) * square
                row = jnp.broadcast_to(rows[m][j : j + 1], rows[m].shape)
                wide_below = jnp.concatenate([below * square] * 2, 1)
                wide_root = jnp.concatenate([root] * 2, 1)
                rows[m] = jnp.where(sub_wide == j, row * wide_root, rows[m] - wide_below * row)
        for m in range(count):
            work[m, pl.ds(start, STRIP), :] = rows[m]
            high = rows[m].astype(jnp.bfloat16).astype(jnp.float32)
            low = rows[m] - high
            after = lane >= start + STRIP
            left_high = jnp.where(after, high[:, :PANEL], 0.0)
            left_low = jnp.where(after, low[:, :PANEL], 0.0)
            left = jnp.concatenate([left_high, left_high, left_low, left_low], 0)
            right = jnp.concatenate([high, low, high, low], 0)
            work[m] = work[m] - lax.dot_general(
                left.T.astype(jnp.bfloat16),
                right.astype(jnp.bfloat16),
                (((1,), (0,)), ((), ())),
                preferred_element_type=jnp.float32,
            )
        return carry

    lax.fori_loop(0, PANEL // STRIP, strip, 0)


def triangle(order):
    return [(p, q) for p in range(order // PANEL) for q in range(p + 1)]


def factor_kernel(diag, factor, packed, inverse, blocks, work):
    count, order = diag.shape[0], diag.shape[2]
    row = lax.broadcasted_iota(jnp.int32, (PANEL, PANEL), 0)
    col = lax.broadcasted_iota(jnp.int32, (PANEL, PANEL), 1)
    eye = jnp.where(row == col, 1.0, 0.0).astype(jnp.float32)
    for m in range(count):
        blocks[m] = diag[m, m]
    inverse[...] = jnp.zeros_like(inverse)
    factor[...] = jnp.zeros_like(factor)
    for start in range(0, order, PANEL):
        stop = start + PANEL
        here = slice(start, stop)
        for m in range(count):
            work[m, :, :PANEL] = blocks[m, here, here]
            work[m, :, PANEL:] = eye
        factor_diagonal(work, count)
        for m in range(count):
            upper = jnp.where(col >= row, work[m, :, :PANEL], 0.0)
            factor[m, here, here] = upper.T
            small = jnp.where(col <= row, work[m, :, PANEL:], 0.0)
            small_parts = split(small)
            if start:
                inverse[m, here, :start] = product(small_parts, split(inverse[m, here, :start]))
            inverse[m, here, here] = small
            if stop < order:
                across = product(small_parts, split(blocks[m, here, stop:]))
                down = across.T
                factor[m, stop:, here] = down
                down_parts = split(down)
                blocks[m, stop:, stop:] -= product(down_parts, split(across))
                inverse[m, stop:, :stop] -= product(down_parts, split(inverse[m, here, :stop]))


    for m in range(count):
        for n, (p, q) in enumerate(triangle(order)):
            tile = inverse[m, p * PANEL : (p + 1) * PANEL, q * PANEL : (q + 1) * PANEL]
            packed[m, 0, n], packed[m, 1, n] = split(tile)


def factored(diag):
    count, order = diag.shape[0], diag.shape[2]
    whole = (count, order, order)
    packed = (count, 2, len(triangle(order)), PANEL, PANEL)
    return pl.pallas_call(
        factor_kernel,
        out_shape=(
            jax.ShapeDtypeStruct(whole, jnp.float32),
            jax.ShapeDtypeStruct(packed, jnp.bfloat16),
        ),
        in_specs=[VMEM],
        out_specs=(VMEM, VMEM),
        scratch_shapes=[
            pltpu.VMEM(whole, jnp.float32),
            pltpu.VMEM(whole, jnp.float32),
            pltpu.VMEM((count, PANEL, 2 * PANEL), jnp.float32),
        ],
        compiler_params=pltpu.CompilerParams(vmem_limit_bytes=40 * 2**20),
        cost_estimate=pl.CostEstimate(
            flops=20_000_000_000, bytes_accessed=3 * diag.size * 4, transcendentals=0
        ),
    )(diag)


def apply_inverse(packed, m, couplings, full, out):
    order = full.shape[1]
    group = 2 * PANEL
    for p in range(order // PANEL - 1):
        corner = (slice(p * PANEL, (p + 1) * PANEL), slice((p + 1) * PANEL, (p + 2) * PANEL))
        full[0, corner[0], corner[1]] = jnp.zeros((PANEL, PANEL), jnp.bfloat16)
        full[1, corner[0], corner[1]] = jnp.zeros((PANEL, PANEL), jnp.bfloat16)
    for n, (p, q) in enumerate(triangle(order)):
        for part in range(2):
            full[part, p * PANEL : (p + 1) * PANEL, q * PANEL : (q + 1) * PANEL] = packed[m, part, n]
    for start in range(0, order, group):
        stop = start + group
        high, low = full[0, start:stop, :stop], full[1, start:stop, :stop]
        for d, coupling in enumerate(couplings):
            right = coupling[:, :stop] if d < 2 else coupling[:stop, :]
            axes = (((1,), (1 if d < 2 else 0,)), ((), ()))
            dot = functools.partial(
                lax.dot_general, dimension_numbers=axes, preferred_element_type=jnp.float32
            )
            out[d, start:stop, :] = (dot(high, right) + dot(low, right)).astype(jnp.bfloat16)


def own_kernel(packed, edge_left, edge_up, horizontal, vertical, out, full):
    first = (edge_left.at[0, 0], edge_up.at[0, 0], horizontal.at[0, 0], vertical.at[0, 0])
    second = (horizontal.at[1, 0], vertical.at[0, 1], horizontal.at[1, 1], vertical.at[1, 1])
    apply_inverse(packed, 0, first, full, out.at[0, 0])
    apply_inverse(packed, 1, second, full, out.at[1, 0])


def below_kernel(packed, left, up, right, out, full):
    couplings = (left.at[0, 0], up.at[1, 0], right.at[0], right.at[1])
    apply_inverse(packed, 0, couplings, full, out.at[0, 0])


def solved_with(kernel, count, operands):
    order = operands[-1].shape[-1]
    flops = 12 * count * order**3
    return pl.pallas_call(
        kernel,
        out_shape=jax.ShapeDtypeStruct((count, 1, 4, order, order), jnp.bfloat16),
        in_specs=[VMEM] * len(operands),
        out_specs=VMEM,
        scratch_shapes=[pltpu.VMEM((2, order, order), jnp.bfloat16)],
        compiler_params=pltpu.CompilerParams(vmem_limit_bytes=40 * 2**20),
        cost_estimate=pl.CostEstimate(
            flops=flops, bytes_accessed=16 * count * order**2, transcendentals=0
        ),
    )(*operands)


def passed_along(value, axis, by):
    size = lax.axis_size(axis)
    return lax.ppermute(value, axis, [(i, (i + by) % size) for i in range(size)])


def select_colour(blocks, parity):
    grid_rows = blocks.shape[0]
    grid_columns = blocks.shape[1]
    trailing = blocks.shape[2:]
    paired = blocks.reshape((grid_rows // 2, 2, grid_columns // 2, 2) + trailing)
    joined = jnp.stack([paired[:, 0, :, parity], paired[:, 1, :, 1 - parity]], 1)
    return joined.reshape((grid_rows, grid_columns // 2) + trailing)


def combine_rows(even_rows, odd_rows):
    joined = jnp.stack([even_rows, odd_rows], 1)
    return joined.reshape((2 * even_rows.shape[0],) + even_rows.shape[1:])


def gram_term(former, latter):
    return jnp.einsum("rmka,rmkb->rmab", former, latter, preferred_element_type=jnp.float32)


def on_device(diag_blocks, horizontal, vertical):
    edge_up = passed_along(vertical[-1:, :1], "row", 1)
    ahead = passed_along(jnp.stack([horizontal[0, 0], vertical[0, 0]]), "row", -1)
    edge_left = passed_along(horizontal[:1, -1:], "col", 1)
    ahead_left = passed_along(edge_left, "row", -1)
    red_factor, packed = factored(diag_blocks)
    below_packed = passed_along(packed[:1], "row", -1)
    solved = solved_with(own_kernel, 2, (packed, edge_left, edge_up, horizontal, vertical))
    red_factor = red_factor[:, None]
    got_above = passed_along(solved[-1:, :, 3], "row", 1)
    above_down = jnp.concatenate([got_above, solved[:-1, :, 3]], 0)
    got_below = solved_with(below_kernel, 1, (below_packed, ahead_left, vertical, ahead))
    below_all = jnp.concatenate([solved[1:], got_below], 0)
    got_left = passed_along(solved[1::2, -1:, 2:4], "col", 1)
    left_pair = combine_rows(
        solved[0::2, :, 2:4], jnp.concatenate([got_left, solved[1::2, :-1, 2:4]], 1)
    )
    right_first, right_rest = passed_along((solved[0::2, :1, 0], solved[0::2, :1, 2:4]), "col", -1)
    right_left = combine_rows(
        jnp.concatenate([solved[0::2, 1:, 0], right_first], 1), solved[1::2, :, 0]
    )
    right_pair = combine_rows(
        jnp.concatenate([solved[0::2, 1:, 2:4], right_rest], 1), solved[1::2, :, 2:4]
    )
    below_up = below_all[:, :, 1]
    update = gram_term(above_down, above_down) + gram_term(below_up, below_up)
    update = (
        update
        + gram_term(left_pair[:, :, 0], left_pair[:, :, 0])
        + gram_term(right_left, right_left)
    )
    black_schur = select_colour(diag_blocks, 1) - update
    east_link = -gram_term(right_left, right_pair[:, :, 0])
    south_link = -gram_term(below_up, below_all[:, :, 3])
    southeast = -(
        gram_term(right_left, right_pair[:, :, 1]) + gram_term(below_up, below_all[:, :, 2])
    )
    southwest = -(
        gram_term(left_pair[:, :, 0], left_pair[:, :, 1]) + gram_term(below_up, below_all[:, :, 0])
    )
    black_links = jnp.stack([east_link, south_link, southeast, southwest], 2).astype(jnp.bfloat16)
    return (red_factor, black_schur, black_links)


def solution(mesh):
    in_specs = (
        P("row", "col", None, None),
        P("row", "col", None, None),
        P("row", "col", None, None),
    )
    out_specs = (
        P("row", "col", None, None),
        P("row", "col", None, None),
        P("row", "col", None, None, None),
    )
    return jax.shard_map(
        on_device, mesh=mesh, in_specs=in_specs, out_specs=out_specs, check_vma=False
    )
```

```python
import functools

import jax
import jax.numpy as jnp
from jax import lax
from jax.experimental import pallas as pl
from jax.experimental.pallas import tpu as pltpu
from jax.sharding import PartitionSpec as P

PANEL = 128
STRIP = 8
VMEM = pl.BlockSpec(memory_space=pltpu.VMEM)


def split(value):
    high = value.astype(jnp.bfloat16)
    low = (value - high.astype(jnp.float32)).astype(jnp.bfloat16)
    return high, low


def product(left, right):
    dot = functools.partial(jnp.dot, preferred_element_type=jnp.float32)
    (lh, ll), (rh, rl) = left, right
    return dot(lh, rh) + (dot(lh, rl) + dot(ll, rh))


def factor_diagonal(work, count):
    lane = lax.broadcasted_iota(jnp.int32, (STRIP, PANEL), 1)
    sub = lax.broadcasted_iota(jnp.int32, (STRIP, PANEL), 0)
    sub_wide = lax.broadcasted_iota(jnp.int32, (STRIP, 2 * PANEL), 0)

    def strip(b, carry):
        start = pl.multiple_of(b * STRIP, STRIP)
        rows = [work[m, pl.ds(start, STRIP), :] for m in range(count)]
        columns = [
            [
                jnp.take_along_axis(rows[m][:, :PANEL], jnp.full_like(lane, start + c), axis=1)
                for c in range(STRIP)
            ]
            for m in range(count)
        ]
        for j in range(STRIP):
            for m in range(count):
                column = columns[m][j]
                pivot = jnp.broadcast_to(column[j : j + 1], column.shape)
                root = lax.rsqrt(pivot)
                square = root * root
                below = jnp.where(sub > j, column, 0.0)
                for c in range(j + 1, STRIP):
                    across = jnp.broadcast_to(columns[m][c][j : j + 1], column.shape)
                    columns[m][c] = columns[m][c] - (below * across) * square
                row = jnp.broadcast_to(rows[m][j : j + 1], rows[m].shape)
                wide_below = jnp.concatenate([below * square] * 2, 1)
                wide_root = jnp.concatenate([root] * 2, 1)
                rows[m] = jnp.where(sub_wide == j, row * wide_root, rows[m] - wide_below * row)
        for m in range(count):
            work[m, pl.ds(start, STRIP), :] = rows[m]
            high = rows[m].astype(jnp.bfloat16).astype(jnp.float32)
            low = rows[m] - high
            after = lane >= start + STRIP
            left_high = jnp.where(after, high[:, :PANEL], 0.0)
            left_low = jnp.where(after, low[:, :PANEL], 0.0)
            left = jnp.concatenate([left_high, left_high, left_low, left_low], 0)
            right = jnp.concatenate([high, low, high, low], 0)
            work[m] = work[m] - lax.dot_general(
                left.T.astype(jnp.bfloat16),
                right.astype(jnp.bfloat16),
                (((1,), (0,)), ((), ())),
                preferred_element_type=jnp.float32,
            )
        return carry

    lax.fori_loop(0, PANEL // STRIP, strip, 0)


def triangle(order):
    return [(p, q) for p in range(order // PANEL) for q in range(p + 1)]


def factor_kernel(diag, factor, packed, inverse, blocks, work):
    count, order = diag.shape[0], diag.shape[2]
    row = lax.broadcasted_iota(jnp.int32, (PANEL, PANEL), 0)
    col = lax.broadcasted_iota(jnp.int32, (PANEL, PANEL), 1)
    eye = jnp.where(row == col, 1.0, 0.0).astype(jnp.float32)
    for m in range(count):
        blocks[m] = diag[m, m]
    inverse[...] = jnp.zeros_like(inverse)
    factor[...] = jnp.zeros_like(factor)
    for start in range(0, order, PANEL):
        stop = start + PANEL
        here = slice(start, stop)
        for m in range(count):
            work[m, :, :PANEL] = blocks[m, here, here]
            work[m, :, PANEL:] = eye
        factor_diagonal(work, count)
        for m in range(count):
            upper = jnp.where(col >= row, work[m, :, :PANEL], 0.0)
            factor[m, here, here] = upper.T
            small = jnp.where(col <= row, work[m, :, PANEL:], 0.0)
            small_parts = split(small)
            if start:
                inverse[m, here, :start] = product(small_parts, split(inverse[m, here, :start]))
            inverse[m, here, here] = small
            if stop < order:
                across = product(small_parts, split(blocks[m, here, stop:]))
                down = across.T
                factor[m, stop:, here] = down
                down_parts = split(down)
                blocks[m, stop:, stop:] -= product(down_parts, split(across))
                inverse[m, stop:, :stop] -= product(down_parts, split(inverse[m, here, :stop]))


    for m in range(count):
        for n, (p, q) in enumerate(triangle(order)):
            tile = inverse[m, p * PANEL : (p + 1) * PANEL, q * PANEL : (q + 1) * PANEL]
            packed[m, 0, n], packed[m, 1, n] = split(tile)


def factored(diag):
    count, order = diag.shape[0], diag.shape[2]
    whole = (count, order, order)
    packed = (count, 2, len(triangle(order)), PANEL, PANEL)
    return pl.pallas_call(
        factor_kernel,
        out_shape=(
            jax.ShapeDtypeStruct(whole, jnp.float32),
            jax.ShapeDtypeStruct(packed, jnp.bfloat16),
        ),
        in_specs=[VMEM],
        out_specs=(VMEM, VMEM),
        scratch_shapes=[
            pltpu.VMEM(whole, jnp.float32),
            pltpu.VMEM(whole, jnp.float32),
            pltpu.VMEM((count, PANEL, 2 * PANEL), jnp.float32),
        ],
        compiler_params=pltpu.CompilerParams(vmem_limit_bytes=40 * 2**20),
        cost_estimate=pl.CostEstimate(
            flops=20_000_000_000, bytes_accessed=3 * diag.size * 4, transcendentals=0
        ),
    )(diag)


def apply_inverse(packed, m, couplings, full, out):
    order = full.shape[1]
    group = 2 * PANEL
    for p in range(order // PANEL - 1):
        corner = (slice(p * PANEL, (p + 1) * PANEL), slice((p + 1) * PANEL, (p + 2) * PANEL))
        full[0, corner[0], corner[1]] = jnp.zeros((PANEL, PANEL), jnp.bfloat16)
        full[1, corner[0], corner[1]] = jnp.zeros((PANEL, PANEL), jnp.bfloat16)
    for n, (p, q) in enumerate(triangle(order)):
        for part in range(2):
            full[part, p * PANEL : (p + 1) * PANEL, q * PANEL : (q + 1) * PANEL] = packed[m, part, n]
    for start in range(0, order, group):
        stop = start + group
        high, low = full[0, start:stop, :stop], full[1, start:stop, :stop]
        for d, coupling in enumerate(couplings):
            right = coupling[:, :stop] if d < 2 else coupling[:stop, :]
            axes = (((1,), (1 if d < 2 else 0,)), ((), ()))
            dot = functools.partial(
                lax.dot_general, dimension_numbers=axes, preferred_element_type=jnp.float32
            )
            out[d, start:stop, :] = (dot(high, right) + dot(low, right)).astype(jnp.bfloat16)


def own_kernel(packed, edge_left, edge_up, horizontal, vertical, out, full):
    first = (edge_left.at[0, 0], edge_up.at[0, 0], horizontal.at[0, 0], vertical.at[0, 0])
    second = (horizontal.at[1, 0], vertical.at[0, 1], horizontal.at[1, 1], vertical.at[1, 1])
    apply_inverse(packed, 0, first, full, out.at[0, 0])
    apply_inverse(packed, 1, second, full, out.at[1, 0])


def below_kernel(packed, left, up, right, out, full):
    couplings = (left.at[0, 0], up.at[1, 0], right.at[0], right.at[1])
    apply_inverse(packed, 0, couplings, full, out.at[0, 0])


def solved_with(kernel, count, operands):
    order = operands[-1].shape[-1]
    flops = 12 * count * order**3
    return pl.pallas_call(
        kernel,
        out_shape=jax.ShapeDtypeStruct((count, 1, 4, order, order), jnp.bfloat16),
        in_specs=[VMEM] * len(operands),
        out_specs=VMEM,
        scratch_shapes=[pltpu.VMEM((2, order, order), jnp.bfloat16)],
        compiler_params=pltpu.CompilerParams(vmem_limit_bytes=40 * 2**20),
        cost_estimate=pl.CostEstimate(
            flops=flops, bytes_accessed=16 * count * order**2, transcendentals=0
        ),
    )(*operands)


def passed_along(value, axis, by):
    size = lax.axis_size(axis)
    return lax.ppermute(value, axis, [(i, (i + by) % size) for i in range(size)])


def passed_diagonally(value):
    rows, columns = lax.axis_size("row"), lax.axis_size("col")
    pairs = [
        (r * columns + c, (r - 1) % rows * columns + (c + 1) % columns)
        for r in range(rows)
        for c in range(columns)
    ]
    return lax.ppermute(value, ("row", "col"), pairs)


def select_colour(blocks, parity):
    grid_rows = blocks.shape[0]
    grid_columns = blocks.shape[1]
    trailing = blocks.shape[2:]
    paired = blocks.reshape((grid_rows // 2, 2, grid_columns // 2, 2) + trailing)
    joined = jnp.stack([paired[:, 0, :, parity], paired[:, 1, :, 1 - parity]], 1)
    return joined.reshape((grid_rows, grid_columns // 2) + trailing)


def combine_rows(even_rows, odd_rows):
    joined = jnp.stack([even_rows, odd_rows], 1)
    return joined.reshape((2 * even_rows.shape[0],) + even_rows.shape[1:])


def gram_term(former, latter):
    return jnp.einsum("rmka,rmkb->rmab", former, latter, preferred_element_type=jnp.float32)


def on_device(diag_blocks, horizontal, vertical):
    edge_up = passed_along(vertical[-1:, :1], "row", 1)
    ahead = passed_along(jnp.stack([horizontal[0, 0], vertical[0, 0]]), "row", -1)
    edge_left = passed_along(horizontal[:1, -1:], "col", 1)
    ahead_left = passed_diagonally(horizontal[:1, -1:])
    red_factor, packed = factored(diag_blocks)
    below_packed = passed_along(packed[:1], "row", -1)
    solved = solved_with(own_kernel, 2, (packed, edge_left, edge_up, horizontal, vertical))
    red_factor = red_factor[:, None]
    got_above = passed_along(solved[-1:, :, 3], "row", 1)
    above_down = jnp.concatenate([got_above, solved[:-1, :, 3]], 0)
    got_below = solved_with(below_kernel, 1, (below_packed, ahead_left, vertical, ahead))
    below_all = jnp.concatenate([solved[1:], got_below], 0)
    got_left = passed_along(solved[1::2, -1:, 2:4], "col", 1)
    left_pair = combine_rows(
        solved[0::2, :, 2:4], jnp.concatenate([got_left, solved[1::2, :-1, 2:4]], 1)
    )
    right_first, right_rest = passed_along((solved[0::2, :1, 0], solved[0::2, :1, 2:4]), "col", -1)
    right_left = combine_rows(
        jnp.concatenate([solved[0::2, 1:, 0], right_first], 1), solved[1::2, :, 0]
    )
    right_pair = combine_rows(
        jnp.concatenate([solved[0::2, 1:, 2:4], right_rest], 1), solved[1::2, :, 2:4]
    )
    below_up = below_all[:, :, 1]
    update = gram_term(above_down, above_down) + gram_term(below_up, below_up)
    update = (
        update
        + gram_term(left_pair[:, :, 0], left_pair[:, :, 0])
        + gram_term(right_left, right_left)
    )
    black_schur = select_colour(diag_blocks, 1) - update
    east_link = -gram_term(right_left, right_pair[:, :, 0])
    south_link = -gram_term(below_up, below_all[:, :, 3])
    southeast = -(
        gram_term(right_left, right_pair[:, :, 1]) + gram_term(below_up, below_all[:, :, 2])
    )
    southwest = -(
        gram_term(left_pair[:, :, 0], left_pair[:, :, 1]) + gram_term(below_up, below_all[:, :, 0])
    )
    black_links = jnp.stack([east_link, south_link, southeast, southwest], 2).astype(jnp.bfloat16)
    return (red_factor, black_schur, black_links)


def solution(mesh):
    in_specs = (
        P("row", "col", None, None),
        P("row", "col", None, None),
        P("row", "col", None, None),
    )
    out_specs = (
        P("row", "col", None, None),
        P("row", "col", None, None),
        P("row", "col", None, None, None),
    )
    return jax.shard_map(
        on_device, mesh=mesh, in_specs=in_specs, out_specs=out_specs, check_vma=False
    )
```
